128 devices in a mesh: row: 8 (over x, y_lo), col: 16 (over z, y_hi, core).
Axes of the slice: x: 4, y: 4 (y_hi: 2, y_lo: 2; y = y_hi * 2 + y_lo), z: 4, core: 2. Of those that a mesh axis runs over, the one named last changes fastest.
Arguments:
- source_blocks: float32 [16384, 24576], P('row', 'col'), may hold values from -6 to 6
Outputs:
- target_blocks: float32 [8192, 49152], P('row', 'col')
- column_sums: float32 [49152], P('col')
- frobenius: float32 [], replicated
The draws below stay inside these ranges and needn't reach their ends.
All inputs are finite; a program needn't handle non-finite values.
Results may differ from the reference program's by a relative error of at most 0.00002.
Values sent between devices are 32-bit elements; how exact they have to be, the bound alone decides.
A program may use at most 128 MiB of HBM per device.

```python
import math
import jax
import jax.numpy as jnp
from jax import lax

N = 24576
SB = 128
RB = 2
TB = 512
M = 16384
E = 6
N_ROW = 8
N_COL = 16


def strengthened(drawn, own_key, source, target, parts, factor):
    owner, partner = [(jnp.arange(drawn.shape[dim]) // (drawn.shape[dim] // parts)).reshape([-1 if axis == dim else 1 for axis in range(drawn.ndim)]) for dim in (source, target)]
    chosen = jax.random.permutation(own_key, parts)[partner]
    strong = (owner == chosen) | (owner == (partner + parts // 2) % parts)
    return jnp.where(strong, factor * drawn, drawn)


def block_scale(key, shape, cuts, smallest, top_value):
    factor_of, own = 1.0, jax.random.fold_in(key, 6)
    for dim, blocks in cuts:
        steps = jnp.exp(jax.random.uniform(jax.random.fold_in(own, dim), (blocks,), jnp.float32, smallest / len(cuts), top_value / len(cuts)))
        factor_of = factor_of * jnp.repeat(steps, shape[dim] // blocks).reshape([-1 if axis == dim else 1 for axis in range(len(shape))])
    return factor_of


def noise_with(own_key, shape, width, bound, split, heavy, held_as=jnp.bfloat16):
    array = width * jax.random.normal(own_key, shape, jnp.float32)
    if split:
        array = array * block_scale(own_key, shape, split, -0.22, 0.18)
    return jnp.clip(strengthened(array, jax.random.fold_in(own_key, 3), *heavy), -bound, bound).astype(held_as)


def setup_inputs(seed: int = 0) -> dict:
    splits = jax.random.split(jax.random.key(seed), 2)
    return {
        "source_blocks": noise_with(splits[0], (M, N), 1.0, 6.0, ((0, 8), (1, 16)), (0, 1, 16, 2.0), jnp.float32),
    }


def reference(source_blocks):
    row_count = N_ROW
    col_count = N_COL
    cells = source_blocks.reshape(row_count, M // row_count // SB, SB, col_count, N // col_count // SB, SB)
    matrix = cells.transpose(1, 0, 2, 4, 3, 5).reshape(M, N)
    pieces = matrix.reshape(RB, 2, 4, row_count // 4, TB, E, 2, col_count // 4, TB)
    target_blocks = pieces.transpose(3, 2, 0, 4, 7, 1, 6, 5, 8).reshape(M // 2, 2 * N)
    scale = 1.0 / math.sqrt(M)
    totals = lax.optimization_barrier(jnp.sum(matrix, axis=0)) * scale
    grouped = totals.reshape(E, 2, col_count // 4, TB).transpose(2, 1, 0, 3)
    column_sums = jnp.broadcast_to(grouped[:, None], (col_count // 4, 2, 2, E, TB)).reshape(2 * N)
    frobenius = jnp.sqrt(jnp.sum(matrix * matrix) / (M * N))
    return (target_blocks, column_sums, frobenius)
```

```python
import functools

import jax
import jax.numpy as jnp
from jax import lax
from jax.experimental import pallas as pl
from jax.experimental.pallas import tpu as pltpu
from jax.sharding import PartitionSpec as P

MESH = pl.DeviceIdType.MESH
ROWS, COLS = 16384, 24576
HALVES, ROW_PARTS, TILES, E, COL_PARTS = 2, 4, 16, 6, 4
F32 = jnp.float32
PARTNERS = [(dx, dy, dc) for dx in (0, 1) for dy in range(4) for dc in (0, 1)][1:]
SLOTS = 4
CHUNKS = HALVES * 8


def exchange(x_ref, o_ref, sums_ref, square_ref, chunk, part, parts, plane, other, mine, squares,
             own_sem, chunk_sem, send_sem, recv_sem, part_send, part_recv, far_send, far_recv, z_send, z_recv):
    row, col = lax.axis_index("row"), lax.axis_index("col")
    x1, x0, y_lo = row // 4, (row // 2) % 2, row % 2
    z, y_hi, core = col // 4, (col // 2) % 2, col % 2
    y = y_hi * 2 + y_lo
    row_part, col_part = x0 * 2 + y_lo, y_hi * 2 + core

    def partner(dx, dy, dc):
        y2 = (y + dy) % 4
        return (x0 + dx) % 2, y2 // 2, y2 % 2, (core + dc) % 2

    def device(p):
        return (x1 * 4 + p[0] * 2 + p[2], z * 4 + p[1] * 2 + p[3])

    across = ((1 - x1) * 4 + (1 - x0) * 2 + y_lo, col)
    stacked = [(row, ((z + dz) % 4) * 4 + col_part) for dz in (1, 2, 3)]
    partners = [partner(*p) for p in PARTNERS]

    barrier = pltpu.get_barrier_semaphore()
    for other_device in [device(p) for p in partners] + [across] + stacked:
        pl.semaphore_signal(barrier, inc=1, device_id=other_device, device_id_type=MESH)
    pl.semaphore_wait(barrier, len(PARTNERS) + 4)

    def bulk(c, i):
        p = partners[i]
        return pltpu.make_async_remote_copy(
            x_ref.at[c, p[1] * 4 + p[0] * 2 + p[2], :, :, p[3]],
            o_ref.at[c, row_part, :, :, col_part],
            send_sem.at[c, i], recv_sem.at[c, i], device_id=device(p), device_id_type=MESH)

    copies = []
    for i in range(len(PARTNERS)):
        copies.append(bulk(0, i))
        copies[-1].start()

    def load(n):
        return pltpu.make_async_copy(x_ref.at[n // 8, n % 8], chunk.at[n % SLOTS], chunk_sem.at[n % SLOTS])

    for n in range(SLOTS - 1):
        load(n).start()
    own = [
        pltpu.make_async_copy(
            x_ref.at[c, y_hi * 4 + row_part, :, :, core], o_ref.at[c, row_part, :, :, col_part], own_sem.at[c])
        for c in range(HALVES)
    ]
    for copy in own:
        copy.start()

    totals = (jnp.zeros((E, 2, 8, 128), F32), jnp.zeros((E, 2, 8, 128), F32))
    for n in range(CHUNKS):
        if n + SLOTS - 1 < CHUNKS:
            load(n + SLOTS - 1).start()
        load(n).wait()

        def add(t, totals, n=n):
            v = chunk[n % SLOTS, t]
            return totals[0] + v, totals[1] + v * v

        totals = lax.fori_loop(0, TILES, add, totals)
    by_column = jnp.sum(totals[0], axis=2)
    square = jnp.sum(totals[1], axis=(0, 1, 2), keepdims=True).reshape(1, 128)
    for c in range(2):
        part[c, 0:E, :] = by_column[:, c]
        part[c, E:E + 1, :] = square
        part[c, E + 1:E + 2, :] = jnp.zeros((1, 128), F32)
    parts[col_part, row_part] = part[core]

    smalls = []
    for i, p in enumerate(partners):
        smalls.append(pltpu.make_async_remote_copy(
            part.at[p[3]], parts.at[col_part, row_part], part_send.at[i], part_recv.at[i],
            device_id=device(p), device_id_type=MESH))
        smalls[-1].start()
    for i in range(len(PARTNERS)):
        copies.append(bulk(1, i))
        copies[-1].start()

    for copy in smalls:
        copy.wait()
    group = parts[:, 0] + parts[:, 1] + parts[:, 2] + parts[:, 3]
    plane[...] = group
    far = pltpu.make_async_remote_copy(plane, other, far_send.at[0], far_recv.at[0], device_id=across, device_id_type=MESH)
    far.start()
    far.wait()
    whole = group + other[...]
    for e in range(E):
        sums_ref[e * COL_PARTS:(e + 1) * COL_PARTS, :] = whole[:, e] * (1.0 / 128.0)
    own_square = jnp.broadcast_to(whole[0, E] + whole[1, E] + whole[2, E] + whole[3, E], (8, 128))
    mine[...] = own_square
    squares[z] = own_square
    hops = [
        pltpu.make_async_remote_copy(mine, squares.at[z], z_send.at[i], z_recv.at[i], device_id=d, device_id_type=MESH)
        for i, d in enumerate(stacked)
    ]
    for copy in hops:
        copy.start()
    for copy in hops:
        copy.wait()
    square_ref[...] = squares[0] + squares[1] + squares[2] + squares[3]

    for copy in own + copies:
        copy.wait()


def write(o_ref, sums_ref, square_ref, out_ref, columns_ref, norm_ref, sem):
    copies = []
    for c in range(HALVES):
        for r in range(ROW_PARTS):
            copies.append(pltpu.make_async_copy(o_ref.at[c, r], out_ref.at[c, r], sem.at[c, r]))
            copies[-1].start()
    columns_ref[...] = sums_ref[...]
    total = jnp.sum(square_ref[0:1, :])
    norm_ref[0, 0] = jnp.max(jnp.sqrt(jnp.full((8, 128), total / (ROWS * COLS), F32)))
    for copy in copies:
        copy.wait()


def solution(mesh):
    big = (HALVES, ROW_PARTS, TILES, E, COL_PARTS, 8, 128)
    vmem = pl.BlockSpec(memory_space=pltpu.VMEM)
    anywhere = pl.BlockSpec(memory_space=pl.ANY)
    n = len(PARTNERS)

    def body(source):
        x = source.reshape(HALVES, 8, TILES, 8, E, 2, 128).transpose(0, 1, 2, 4, 5, 3, 6)
        o, sums, square = pl.pallas_call(
            exchange,
            name="exchange",
            out_shape=(pltpu.VMEM(big, F32), pltpu.VMEM((E * COL_PARTS, 128), F32), pltpu.VMEM((8, 128), F32)),
            in_specs=[anywhere],
            out_specs=(vmem, vmem, vmem),
            scratch_shapes=[
                pltpu.VMEM((SLOTS, TILES, E, 2, 8, 128), F32),
                pltpu.VMEM((2, 8, 128), F32),
                pltpu.VMEM((COL_PARTS, ROW_PARTS, 8, 128), F32),
                pltpu.VMEM((COL_PARTS, 8, 128), F32),
                pltpu.VMEM((COL_PARTS, 8, 128), F32),
                pltpu.VMEM((8, 128), F32),
                pltpu.VMEM((4, 8, 128), F32),
                pltpu.SemaphoreType.DMA((HALVES,)),
                pltpu.SemaphoreType.DMA((SLOTS,)),
                pltpu.SemaphoreType.DMA((HALVES, n)),
                pltpu.SemaphoreType.DMA((HALVES, n)),
                pltpu.SemaphoreType.DMA((n,)),
                pltpu.SemaphoreType.DMA((n,)),
                pltpu.SemaphoreType.DMA((1,)),
                pltpu.SemaphoreType.DMA((1,)),
                pltpu.SemaphoreType.DMA((3,)),
                pltpu.SemaphoreType.DMA((3,)),
            ],
            compiler_params=pltpu.CompilerParams(collective_id=0, has_side_effects=True, vmem_limit_bytes=40 << 20),
        )(x)
        out, columns, norm = pl.pallas_call(
            write,
            name="write",
            out_shape=(jax.ShapeDtypeStruct(big, F32), jax.ShapeDtypeStruct((E * COL_PARTS, 128), F32),
                       jax.ShapeDtypeStruct((1, 1), F32)),
            in_specs=[vmem, vmem, vmem],
            out_specs=(anywhere, vmem, pl.BlockSpec(memory_space=pltpu.SMEM)),
            scratch_shapes=[pltpu.SemaphoreType.DMA((HALVES, ROW_PARTS))],
            compiler_params=pltpu.CompilerParams(vmem_limit_bytes=40 << 20),
        )(o, sums, square)
        return out.transpose(0, 1, 2, 5, 3, 4, 6).reshape(1024, 3072), columns.reshape(3072), norm.reshape(())

    return jax.shard_map(body, mesh=mesh, in_specs=P("row", "col"), out_specs=(P("row", "col"), P("col"), P()),
                         check_vma=False)
```

```python
import functools

import jax
import jax.numpy as jnp
from jax import lax
from jax.experimental import pallas as pl
from jax.experimental.pallas import tpu as pltpu
from jax.sharding import PartitionSpec as P


AXES = ("row", "col")
ROWS, COLS = 16384, 24576
N_ROW, N_COL = 8, 16
HALVES, ROW_PARTS, TILES, E, COL_PARTS = 2, 4, 16, 6, 4
F32 = jnp.float32
WHOLE, UPPER, LOWER = (0, 1), (0,), (1,)
FIRST = [(1, 0, 0, WHOLE), (0, 1, 0, WHOLE), (0, 3, 0, WHOLE)]
SECOND = [(1, 0, 1, WHOLE), (0, 1, 1, UPPER), (0, 3, 1, UPPER)]
THIRD = [(1, 1, 0, WHOLE), (0, 1, 1, LOWER), (0, 3, 1, LOWER), (0, 2, 0, WHOLE), (0, 2, 1, WHOLE), (1, 3, 0, WHOLE),
         (1, 1, 1, WHOLE), (1, 3, 1, WHOLE), (0, 0, 1, WHOLE), (1, 2, 0, WHOLE), (1, 2, 1, WHOLE)]
NEAR = [(0, 1, 0), (0, 3, 0), (0, 2, 0), (1, 0, 0), (1, 1, 0), (1, 3, 0), (1, 2, 0)]
LATE = [(0, 1, 1, LOWER), (0, 3, 1, LOWER), (0, 2, 0, WHOLE), (0, 2, 1, WHOLE), (1, 2, 1, WHOLE)]
MIDDLE = [(1, 2, 0, WHOLE)]
SOON = [f for f in FIRST + SECOND + THIRD if f not in LATE + MIDDLE]
SLOTS = 4
CHUNKS = HALVES * 8
VMEM = pl.BlockSpec(memory_space=pltpu.VMEM)
HBM = pl.BlockSpec(memory_space=pltpu.HBM)
SMALL = (8, 128)
BIG = (HALVES, ROW_PARTS, TILES, E, COL_PARTS, 8, 128)


def place(row, col):
    return {"x1": row // 4, "x0": (row // 2) % 2, "y": (col // 2) % 2 * 2 + row % 2, "z": col // 4, "core": col % 2}


def here():
    return place(lax.axis_index("row"), lax.axis_index("col"))


def shifted(at, flow, sign):
    dx, dy, dc = flow[:3]
    core = (at["core"] + dc) % 2
    turn = 1 - 2 * (at["core"] if sign > 0 else core)
    return at | {"x0": (at["x0"] + dx) % 2, "y": (at["y"] + sign * turn * dy + 4) % 4, "core": core}


def device(at):
    return at["x1"] * 4 + at["x0"] * 2 + at["y"] % 2, at["z"] * 4 + at["y"] // 2 * 2 + at["core"]


def row_part(at):
    return at["x0"] * 2 + at["y"] % 2


def col_part(at):
    return at["y"] // 2 * 2 + at["core"]


def slab(at):
    return at["y"] // 2 * 4 + at["x0"] * 2 + at["y"] % 2


def moved(target):
    pairs = []
    for row in range(N_ROW):
        for col in range(N_COL):
            to_row, to_col = device(target(place(row, col)))
            pairs.append((row * N_COL + col, to_row * N_COL + to_col))
    return pairs


def permutation(flow):
    return moved(lambda at: shifted(at, flow, 1))


def half(piece, i):
    return piece.at[i * TILES:(i + 1) * TILES]


def pack(flows, x_ref, *refs):
    n = len(flows)
    sem, outs = refs[-1], refs[len(refs) - 1 - n:-1]
    at = here()
    copies = []
    for k, flow in enumerate(flows):
        to = shifted(at, flow, 1)
        for i, c in enumerate(flow[3]):
            copies.append(pltpu.make_async_copy(x_ref.at[c, slab(to), :, :, to["core"]], half(outs[k], i), sem.at[i, k]))
            copies[-1].start()
    for copy in copies:
        copy.wait()


def reduce(x_ref, _, part_ref, chunk, sem):
    def load(n):
        return pltpu.make_async_copy(x_ref.at[n // 8, n % 8], chunk.at[n % SLOTS], sem.at[n % SLOTS])

    for n in range(SLOTS - 1):
        load(n).start()
    totals = (jnp.zeros((E, 2, 8, 128), F32), jnp.zeros((E, 2, 8, 128), F32))
    for n in range(CHUNKS):
        if n + SLOTS - 1 < CHUNKS:
            load(n + SLOTS - 1).start()
        load(n).wait()

        def add(t, totals, n=n):
            v = chunk[n % SLOTS, t]
            return totals[0] + v, totals[1] + v * v

        totals = lax.fori_loop(0, TILES, add, totals)
    by_column = jnp.sum(totals[0], axis=2)
    square = jnp.sum(totals[1], axis=(0, 1, 2), keepdims=True).reshape(1, 128)
    for c in range(2):
        part_ref[c, 0:E, :] = by_column[:, c]
        part_ref[c, E:E + 1, :] = square
        part_ref[c, E + 1:E + 2, :] = jnp.zeros((1, 128), F32)


def write(at, flows, pieces, out_ref, sem):
    copies = []
    for k, flow in enumerate(flows):
        by = shifted(at, flow, -1)
        for i, c in enumerate(flow[3]):
            copies.append(pltpu.make_async_copy(
                half(pieces[k], i), out_ref.at[c, row_part(by), :, :, col_part(by)], sem.at[i, k]))
            copies[-1].start()
    return copies


def pair(part, twin, both_ref):
    core = lax.axis_index("col") % 2
    both_ref[0] = part[core]
    both_ref[1] = twin[core]


def gather(*refs):
    plane_ref, parts = refs[-2:]
    at = here()
    for flow, both in zip([(0, 0, 0)] + NEAR, refs):
        by = shifted(at, flow, -1)
        parts[col_part(by), row_part(by)] = both[0]
        parts[col_part(by | {"core": 1 - at["core"]}), row_part(by)] = both[1]
    plane_ref[...] = parts[:, 0] + parts[:, 1] + parts[:, 2] + parts[:, 3]


def write_soon(x_ref, *refs):
    n = len(SOON)
    pieces, (out_ref, own, own_sem, sem) = refs[:n], refs[n:]
    at = here()
    load = pltpu.make_async_copy(x_ref.at[:, slab(at), :, :, at["core"]], own, own_sem.at[0])
    load.start()
    copies = write(at, SOON, pieces, out_ref, sem)
    load.wait()
    copies.append(pltpu.make_async_copy(own, out_ref.at[:, row_part(at), :, :, col_part(at)], own_sem.at[1]))
    copies[-1].start()
    for copy in copies:
        copy.wait()


def write_middle(_, *refs):
    n = len(MIDDLE)
    pieces, (out_ref, sem) = refs[:n], refs[n:]
    for copy in write(here(), MIDDLE, pieces, out_ref, sem):
        copy.wait()


def combine(plane_ref, other_ref, sums_ref, square_ref):
    whole = plane_ref[...] + other_ref[...]
    for e in range(E):
        sums_ref[e * COL_PARTS:(e + 1) * COL_PARTS, :] = whole[:, e] * (1.0 / 128.0)
    square_ref[...] = jnp.broadcast_to(whole[0, E] + whole[1, E] + whole[2, E] + whole[3, E], SMALL)


def write_late(_, sums_ref, square_ref, z1, z2, z3, *refs):
    n = len(LATE)
    pieces, (out_ref, columns_ref, norm_ref, squares, sem) = refs[:n], refs[n:]
    at = here()
    copies = write(at, LATE, pieces, out_ref, sem)
    columns_ref[...] = sums_ref[...]
    for dz, ref in enumerate((square_ref, z1, z2, z3)):
        squares[(at["z"] - dz + 4) % 4] = ref[...]
    total = jnp.sum((squares[0] + squares[1] + squares[2] + squares[3])[0:1, :])
    norm_ref[0, 0] = jnp.max(jnp.sqrt(jnp.full(SMALL, total / (ROWS * COLS), F32)))
    for copy in copies:
        copy.wait()


FLOPS_PER_US = 10_000_000


def plain(kernel, outs, in_specs, out_specs, scratch, us, **kw):
    return pl.pallas_call(
        kernel, out_shape=outs, in_specs=in_specs, out_specs=out_specs, scratch_shapes=scratch,
        cost_estimate=pl.CostEstimate(flops=int(us * FLOPS_PER_US), bytes_accessed=1 << 20, transcendentals=0),
        compiler_params=pltpu.CompilerParams(vmem_limit_bytes=12 << 20), **kw)


def body(source):
    dma = pltpu.SemaphoreType.DMA
    x = source.reshape(HALVES, 8, TILES, 8, E, 2, 128).transpose(0, 1, 2, 4, 5, 3, 6)
    x = pltpu.with_memory_space_constraint(x, pltpu.HBM)
    landed = {}

    def permute(value, pairs):
        return lax.ppermute(value, AXES, pairs)

    def go(flows, *before):
        n = len(flows)
        pieces = plain(
            functools.partial(pack, flows), tuple(pltpu.VMEM((len(f[3]) * TILES, E, 8, 128), F32) for f in flows),
            [HBM] + [VMEM] * len(before), (VMEM,) * n, [dma((HALVES, n))], 1 + n / 3)(x, *before)
        for flow, piece in zip(flows, pieces):
            landed[flow] = permute(piece, permutation(flow))
        return pieces

    pieces = go(FIRST)
    pieces = go(SECOND, pieces[0])
    pieces = go(THIRD, pieces[0])
    tiles = functools.partial(pltpu.VMEM, dtype=F32)
    part = plain(reduce, tiles((2, *SMALL)), [HBM, VMEM], VMEM,
                 [pltpu.VMEM((SLOTS, TILES, E, 2, 8, 128), F32), dma((SLOTS,))], 7)(x, pieces[0])
    twin = permute(part, permutation((0, 0, 1)))
    both = plain(pair, tiles((2, *SMALL)), [VMEM] * 2, VMEM, [], 1)(part, twin)
    near = [permute(both, permutation(f)) for f in NEAR]
    plane = plain(gather, tiles((COL_PARTS, *SMALL)), [VMEM] * (1 + len(NEAR)), VMEM,
                  [tiles((COL_PARTS, ROW_PARTS, *SMALL))], 1)(both, *near)
    other = permute(plane, moved(lambda at: at | {"x1": 1 - at["x1"], "x0": 1 - at["x0"]}))
    sums, square = plain(
        combine, (tiles((E * COL_PARTS, 128)), tiles(SMALL)), [VMEM] * 2, (VMEM,) * 2, [], 1)(plane, other)
    stacked = [
        permute(square, moved(lambda at: at | {"z": (at["z"] + dz) % 4})) for dz in (1, 2, 3)]
    n = len(SOON)
    out = plain(
        write_soon, jax.ShapeDtypeStruct(BIG, F32), [HBM] + [VMEM] * n, HBM,
        [pltpu.VMEM((HALVES, TILES, E, 8, 128), F32), dma((2,)), dma((HALVES, n))], 5,
    )(x, *[landed[f] for f in SOON])
    n = len(MIDDLE)
    out = plain(
        write_middle, jax.ShapeDtypeStruct(BIG, F32), [HBM] + [VMEM] * n, HBM,
        [dma((HALVES, n))], 2, input_output_aliases={0: 0})(out, *[landed[f] for f in MIDDLE])
    n = len(LATE)
    out, columns, norm = plain(
        write_late,
        (jax.ShapeDtypeStruct(BIG, F32), jax.ShapeDtypeStruct((E * COL_PARTS, 128), F32),
         jax.ShapeDtypeStruct((1, 1), F32)),
        [HBM] + [VMEM] * (n + 5), (HBM, VMEM, pl.BlockSpec(memory_space=pltpu.SMEM)),
        [pltpu.VMEM((4, *SMALL), F32), dma((HALVES, n))], 2, input_output_aliases={0: 0},
    )(out, sums, square, *stacked, *[landed[f] for f in LATE])
    return out.transpose(0, 1, 2, 5, 3, 4, 6).reshape(1024, 3072), columns.reshape(3072), norm.reshape(())


def solution(mesh):
    return jax.shard_map(body, mesh=mesh, in_specs=P("row", "col"), out_specs=(P("row", "col"), P("col"), P()),
                         check_vma=False)
```

```python
import functools

import jax
import jax.numpy as jnp
from jax import lax
from jax.experimental import pallas as pl
from jax.experimental.pallas import tpu as pltpu
from jax.sharding import PartitionSpec as P


AXES = ("row", "col")
ROWS, COLS = 16384, 24576
N_ROW, N_COL = 8, 16
HALVES, ROW_PARTS, TILES, E, COL_PARTS = 2, 4, 16, 6, 4
F32 = jnp.float32
WHOLE, UPPER, LOWER = (0, 1), (0,), (1,)
FIRST = [(1, 0, 0, WHOLE), (0, 1, 0, WHOLE)]
SECOND = [(0, 3, 0, WHOLE), (1, 0, 1, WHOLE), (0, 1, 1, UPPER), (0, 3, 1, UPPER)]
THIRD = [(1, 1, 0, WHOLE), (0, 1, 1, LOWER), (0, 3, 1, LOWER), (0, 2, 0, WHOLE), (0, 2, 1, WHOLE), (1, 3, 0, WHOLE),
         (1, 1, 1, WHOLE), (1, 3, 1, WHOLE), (0, 0, 1, WHOLE), (1, 2, 0, WHOLE), (1, 2, 1, WHOLE)]
NEAR = [(0, 1, 0), (0, 3, 0), (0, 2, 0), (1, 0, 0), (1, 1, 0), (1, 3, 0), (1, 2, 0)]
GROUPS = [[(1, 2, 0, WHOLE)], [(0, 1, 1, LOWER), (0, 3, 1, LOWER), (0, 2, 0, WHOLE)], [(0, 2, 1, WHOLE), (1, 2, 1, WHOLE)]]
SOON = [f for f in FIRST + SECOND + THIRD if f not in sum(GROUPS, [])]
SLOTS = 4
CHUNKS = HALVES * 8
VMEM = pl.BlockSpec(memory_space=pltpu.VMEM)
HBM = pl.BlockSpec(memory_space=pltpu.HBM)
SMALL = (8, 128)
BIG = (HALVES, ROW_PARTS, TILES, E, COL_PARTS, 8, 128)


def place(row, col):
    return {"x1": row // 4, "x0": (row // 2) % 2, "y": (col // 2) % 2 * 2 + row % 2, "z": col // 4, "core": col % 2}


def here():
    return place(lax.axis_index("row"), lax.axis_index("col"))


def shifted(at, flow, sign):
    dx, dy, dc = flow[:3]
    core = (at["core"] + dc) % 2
    turn = 1 - 2 * (at["core"] if sign > 0 else core)
    return at | {"x0": (at["x0"] + dx) % 2, "y": (at["y"] + sign * turn * dy + 4) % 4, "core": core}


def device(at):
    return at["x1"] * 4 + at["x0"] * 2 + at["y"] % 2, at["z"] * 4 + at["y"] // 2 * 2 + at["core"]


def row_part(at):
    return at["x0"] * 2 + at["y"] % 2


def col_part(at):
    return at["y"] // 2 * 2 + at["core"]


def slab(at):
    return at["y"] // 2 * 4 + at["x0"] * 2 + at["y"] % 2


def moved(target):
    pairs = []
    for row in range(N_ROW):
        for col in range(N_COL):
            to_row, to_col = device(target(place(row, col)))
            pairs.append((row * N_COL + col, to_row * N_COL + to_col))
    return pairs


def permutation(flow):
    return moved(lambda at: shifted(at, flow, 1))


def half(piece, i):
    return piece.at[i * TILES:(i + 1) * TILES]


def pack(flows, x_ref, *refs):
    n = len(flows)
    sem, outs = refs[-1], refs[len(refs) - 1 - n:-1]
    at = here()
    copies = []
    for k, flow in enumerate(flows):
        to = shifted(at, flow, 1)
        for i, c in enumerate(flow[3]):
            copies.append(pltpu.make_async_copy(x_ref.at[c, slab(to), :, :, to["core"]], half(outs[k], i), sem.at[i, k]))
            copies[-1].start()
    for copy in copies:
        copy.wait()


def reduce(x_ref, _, part_ref, chunk, sem):
    def load(n):
        return pltpu.make_async_copy(x_ref.at[n // 8, n % 8], chunk.at[n % SLOTS], sem.at[n % SLOTS])

    for n in range(SLOTS - 1):
        load(n).start()
    totals = (jnp.zeros((E, 2, 8, 128), F32), jnp.zeros((E, 2, 8, 128), F32))
    for n in range(CHUNKS):
        if n + SLOTS - 1 < CHUNKS:
            load(n + SLOTS - 1).start()
        load(n).wait()

        def add(t, totals, n=n):
            v = chunk[n % SLOTS, t]
            return totals[0] + v, totals[1] + v * v

        totals = lax.fori_loop(0, TILES, add, totals)
    by_column = jnp.sum(totals[0], axis=2)
    square = jnp.sum(totals[1], axis=(0, 1, 2), keepdims=True).reshape(1, 128)
    for c in range(2):
        part_ref[c, 0:E, :] = by_column[:, c]
        part_ref[c, E:E + 1, :] = square
        part_ref[c, E + 1:E + 2, :] = jnp.zeros((1, 128), F32)


def write(at, flows, pieces, out_ref, sem):
    copies = []
    for k, flow in enumerate(flows):
        by = shifted(at, flow, -1)
        for i, c in enumerate(flow[3]):
            copies.append(pltpu.make_async_copy(
                half(pieces[k], i), out_ref.at[c, row_part(by), :, :, col_part(by)], sem.at[i, k]))
            copies[-1].start()
    return copies


def pair(part, twin, both_ref):
    core = lax.axis_index("col") % 2
    both_ref[0] = part[core]
    both_ref[1] = twin[core]


def gather(*refs):
    plane_ref, parts = refs[-2:]
    at = here()
    for flow, both in zip([(0, 0, 0)] + NEAR, refs):
        by = shifted(at, flow, -1)
        parts[col_part(by), row_part(by)] = both[0]
        parts[col_part(by | {"core": 1 - at["core"]}), row_part(by)] = both[1]
    plane_ref[...] = parts[:, 0] + parts[:, 1] + parts[:, 2] + parts[:, 3]


def write_soon(x_ref, *refs):
    n = len(SOON)
    pieces, (out_ref, own, own_sem, sem) = refs[:n], refs[n:]
    at = here()
    load = pltpu.make_async_copy(x_ref.at[:, slab(at), :, :, at["core"]], own, own_sem.at[0])
    load.start()
    copies = write(at, SOON, pieces, out_ref, sem)
    load.wait()
    copies.append(pltpu.make_async_copy(own, out_ref.at[:, row_part(at), :, :, col_part(at)], own_sem.at[1]))
    copies[-1].start()
    for copy in copies:
        copy.wait()


def write_group(flows, _, *refs):
    pieces, (out_ref, sem) = refs[:len(flows)], refs[len(flows):]
    for copy in write(here(), flows, pieces, out_ref, sem):
        copy.wait()


def combine(plane_ref, other_ref, sums_ref, square_ref):
    whole = plane_ref[...] + other_ref[...]
    for e in range(E):
        sums_ref[e * COL_PARTS:(e + 1) * COL_PARTS, :] = whole[:, e] * (1.0 / 128.0)
    square_ref[...] = jnp.broadcast_to(whole[0, E] + whole[1, E] + whole[2, E] + whole[3, E], SMALL)


def finish(sums_ref, square_ref, z1, z2, z3, columns_ref, norm_ref, squares):
    z = lax.axis_index("col") // 4
    columns_ref[...] = sums_ref[...]
    for dz, ref in enumerate((square_ref, z1, z2, z3)):
        squares[(z - dz + 4) % 4] = ref[...]
    total = jnp.sum((squares[0] + squares[1] + squares[2] + squares[3])[0:1, :])
    norm_ref[0, 0] = jnp.max(jnp.sqrt(jnp.full(SMALL, total / (ROWS * COLS), F32)))


FLOPS_PER_US = 10_000_000


def plain(kernel, outs, in_specs, out_specs, scratch, us, **kw):
    return pl.pallas_call(
        kernel, out_shape=outs, in_specs=in_specs, out_specs=out_specs, scratch_shapes=scratch,
        cost_estimate=pl.CostEstimate(flops=int(us * FLOPS_PER_US), bytes_accessed=1 << 20, transcendentals=0),
        compiler_params=pltpu.CompilerParams(vmem_limit_bytes=12 << 20), **kw)


def body(source):
    dma = pltpu.SemaphoreType.DMA
    x = source.reshape(HALVES, 8, TILES, 8, E, 2, 128).transpose(0, 1, 2, 4, 5, 3, 6)
    x = pltpu.with_memory_space_constraint(x, pltpu.HBM)
    landed = {}

    def permute(value, pairs):
        return lax.ppermute(value, AXES, pairs)

    def go(flows, *before):
        n = len(flows)
        pieces = plain(
            functools.partial(pack, flows), tuple(pltpu.VMEM((len(f[3]) * TILES, E, 8, 128), F32) for f in flows),
            [HBM] + [VMEM] * len(before), (VMEM,) * n, [dma((HALVES, n))], 1 + n / 3)(x, *before)
        for flow, piece in zip(flows, pieces):
            landed[flow] = permute(piece, permutation(flow))
        return pieces

    pieces = go(FIRST)
    pieces = go(SECOND, pieces[0])
    pieces = go(THIRD, pieces[0])
    tiles = functools.partial(pltpu.VMEM, dtype=F32)
    part = plain(reduce, tiles((2, *SMALL)), [HBM, VMEM], VMEM,
                 [pltpu.VMEM((SLOTS, TILES, E, 2, 8, 128), F32), dma((SLOTS,))], 7)(x, pieces[0])
    twin = permute(part, permutation((0, 0, 1)))
    both = plain(pair, tiles((2, *SMALL)), [VMEM] * 2, VMEM, [], 1)(part, twin)
    near = [permute(both, permutation(f)) for f in NEAR]
    plane = plain(gather, tiles((COL_PARTS, *SMALL)), [VMEM] * (1 + len(NEAR)), VMEM,
                  [tiles((COL_PARTS, ROW_PARTS, *SMALL))], 1)(both, *near)
    other = permute(plane, moved(lambda at: at | {"x1": 1 - at["x1"], "x0": 1 - at["x0"]}))
    sums, square = plain(
        combine, (tiles((E * COL_PARTS, 128)), tiles(SMALL)), [VMEM] * 2, (VMEM,) * 2, [], 1)(plane, other)
    stacked = [
        permute(square, moved(lambda at: at | {"z": (at["z"] + dz) % 4})) for dz in (1, 2, 3)]
    n = len(SOON)
    out = plain(
        write_soon, jax.ShapeDtypeStruct(BIG, F32), [HBM] + [VMEM] * n, HBM,
        [pltpu.VMEM((HALVES, TILES, E, 8, 128), F32), dma((2,)), dma((HALVES, n))], 5,
    )(x, *[landed[f] for f in SOON])
    columns, norm = plain(
        finish, (jax.ShapeDtypeStruct((E * COL_PARTS, 128), F32), jax.ShapeDtypeStruct((1, 1), F32)),
        [VMEM] * 5, (VMEM, pl.BlockSpec(memory_space=pltpu.SMEM)), [tiles((4, *SMALL))], 1)(sums, square, *stacked)
    for flows in GROUPS:
        n = len(flows)
        out = plain(
            functools.partial(write_group, flows), jax.ShapeDtypeStruct(BIG, F32), [HBM] + [VMEM] * n, HBM,
            [dma((HALVES, n))], 1, input_output_aliases={0: 0})(out, *[landed[f] for f in flows])
    return out.transpose(0, 1, 2, 5, 3, 4, 6).reshape(1024, 3072), columns.reshape(3072), norm.reshape(())


def solution(mesh):
    return jax.shard_map(body, mesh=mesh, in_specs=P("row", "col"), out_specs=(P("row", "col"), P("col"), P()),
                         check_vma=False)
```

```python
import functools

import jax
import jax.numpy as jnp
from jax import lax
from jax.experimental import pallas as pl
from jax.experimental.pallas import tpu as pltpu
from jax.sharding import PartitionSpec as P


AXES = ("row", "col")
ROWS, COLS = 16384, 24576
N_ROW, N_COL = 8, 16
HALVES, ROW_PARTS, TILES, E, COL_PARTS = 2, 4, 16, 6, 4
F32 = jnp.float32
WHOLE = (0, 1)
FIRST = [(1, 2, 0, WHOLE), (0, 1, 0, WHOLE)]
SECOND = [(0, 3, 0, WHOLE)]
THIRD = [(1, 1, 0, WHOLE), (1, 3, 0, WHOLE), (0, 1, 1, WHOLE), (0, 3, 1, WHOLE), (1, 1, 1, WHOLE), (0, 2, 0, WHOLE), (0, 2, 1, WHOLE), (1, 3, 1, WHOLE), (0, 0, 1, WHOLE), (1, 2, 1, WHOLE), (1, 0, 0, WHOLE), (1, 0, 1, WHOLE)]
NEAR = [(0, 1, 0), (0, 3, 0), (0, 2, 0), (1, 0, 0), (1, 1, 0), (1, 3, 0), (1, 2, 0)]
GROUPS = [[(1, 0, 0, WHOLE), (0, 1, 1, WHOLE)], [(0, 3, 1, WHOLE), (0, 2, 0, WHOLE), (0, 2, 1, WHOLE), (1, 0, 1, WHOLE)]]
SOON = [f for f in FIRST + SECOND + THIRD if f not in sum(GROUPS, [])]
SLOTS = 4
CHUNKS = HALVES * 8
VMEM = pl.BlockSpec(memory_space=pltpu.VMEM)
HBM = pl.BlockSpec(memory_space=pltpu.HBM)
SMALL = (8, 128)
BIG = (HALVES, ROW_PARTS, TILES, E, COL_PARTS, 8, 128)


def place(row, col):
    return {"x1": row // 4, "x0": (row // 2) % 2, "y": (col // 2) % 2 * 2 + row % 2, "z": col // 4, "core": col % 2}


def here():
    return place(lax.axis_index("row"), lax.axis_index("col"))


def shifted(at, flow, sign):
    dx, dy, dc = flow[:3]
    core = (at["core"] + dc) % 2
    turn = 1 - 2 * (at["core"] if sign > 0 else core)
    return at | {"x0": (at["x0"] + dx) % 2, "y": (at["y"] + sign * turn * dy + 4) % 4, "core": core}


def device(at):
    return at["x1"] * 4 + at["x0"] * 2 + at["y"] % 2, at["z"] * 4 + at["y"] // 2 * 2 + at["core"]


def row_part(at):
    return at["x0"] * 2 + at["y"] % 2


def col_part(at):
    return at["y"] // 2 * 2 + at["core"]


def slab(at):
    return at["y"] // 2 * 4 + at["x0"] * 2 + at["y"] % 2


def moved(target):
    pairs = []
    for row in range(N_ROW):
        for col in range(N_COL):
            to_row, to_col = device(target(place(row, col)))
            pairs.append((row * N_COL + col, to_row * N_COL + to_col))
    return pairs


def permutation(flow):
    return moved(lambda at: shifted(at, flow, 1))


def half(piece, i):
    return piece.at[i * TILES:(i + 1) * TILES]


def pack(flows, x_ref, *refs):
    n = len(flows)
    sem, outs = refs[-1], refs[len(refs) - 1 - n:-1]
    at = here()
    copies = []
    for k, flow in enumerate(flows):
        to = shifted(at, flow, 1)
        for i, c in enumerate(flow[3]):
            copies.append(pltpu.make_async_copy(x_ref.at[c, slab(to), :, :, to["core"]], half(outs[k], i), sem.at[i, k]))
            copies[-1].start()
    for copy in copies:
        copy.wait()


def reduce(x_ref, _, part_ref, chunk, sem):
    def load(n):
        return pltpu.make_async_copy(x_ref.at[n // 8, n % 8], chunk.at[n % SLOTS], sem.at[n % SLOTS])

    for n in range(SLOTS - 1):
        load(n).start()
    totals = (jnp.zeros((E, 2, 8, 128), F32), jnp.zeros((E, 2, 8, 128), F32))
    for n in range(CHUNKS):
        if n + SLOTS - 1 < CHUNKS:
            load(n + SLOTS - 1).start()
        load(n).wait()

        def add(t, totals, n=n):
            v = chunk[n % SLOTS, t]
            return totals[0] + v, totals[1] + v * v

        totals = lax.fori_loop(0, TILES, add, totals)
    by_column = jnp.sum(totals[0], axis=2)
    square = jnp.sum(totals[1], axis=(0, 1, 2), keepdims=True).reshape(1, 128)
    for c in range(2):
        part_ref[c, 0:E, :] = by_column[:, c]
        part_ref[c, E:E + 1, :] = square
        part_ref[c, E + 1:E + 2, :] = jnp.zeros((1, 128), F32)


def write(at, flows, pieces, out_ref, sem):
    copies = []
    for k, flow in enumerate(flows):
        by = shifted(at, flow, -1)
        for i, c in enumerate(flow[3]):
            copies.append(pltpu.make_async_copy(
                half(pieces[k], i), out_ref.at[c, row_part(by), :, :, col_part(by)], sem.at[i, k]))
            copies[-1].start()
    return copies


def pair(part, twin, both_ref):
    core = lax.axis_index("col") % 2
    both_ref[0] = part[core]
    both_ref[1] = twin[core]


def gather(*refs):
    plane_ref, parts = refs[-2:]
    at = here()
    for flow, both in zip([(0, 0, 0)] + NEAR, refs):
        by = shifted(at, flow, -1)
        parts[col_part(by), row_part(by)] = both[0]
        parts[col_part(by | {"core": 1 - at["core"]}), row_part(by)] = both[1]
    plane_ref[...] = parts[:, 0] + parts[:, 1] + parts[:, 2] + parts[:, 3]


def write_soon(x_ref, *refs):
    n = len(SOON)
    pieces, (out_ref, own, own_sem, sem) = refs[:n], refs[n:]
    at = here()
    load = pltpu.make_async_copy(x_ref.at[:, slab(at), :, :, at["core"]], own, own_sem.at[0])
    load.start()
    copies = write(at, SOON, pieces, out_ref, sem)
    load.wait()
    copies.append(pltpu.make_async_copy(own, out_ref.at[:, row_part(at), :, :, col_part(at)], own_sem.at[1]))
    copies[-1].start()
    for copy in copies:
        copy.wait()


def write_group(flows, _, *refs):
    pieces, (out_ref, sem) = refs[:len(flows)], refs[len(flows):]
    for copy in write(here(), flows, pieces, out_ref, sem):
        copy.wait()


def combine(plane_ref, other_ref, sums_ref, square_ref):
    whole = plane_ref[...] + other_ref[...]
    for e in range(E):
        sums_ref[e * COL_PARTS:(e + 1) * COL_PARTS, :] = whole[:, e] * (1.0 / 128.0)
    square_ref[...] = jnp.broadcast_to(whole[0, E] + whole[1, E] + whole[2, E] + whole[3, E], SMALL)


def finish(sums_ref, square_ref, z1, z2, z3, columns_ref, norm_ref, squares):
    z = lax.axis_index("col") // 4
    columns_ref[...] = sums_ref[...]
    for dz, ref in enumerate((square_ref, z1, z2, z3)):
        squares[(z - dz + 4) % 4] = ref[...]
    total = jnp.sum((squares[0] + squares[1] + squares[2] + squares[3])[0:1, :])
    norm_ref[0, 0] = jnp.max(jnp.sqrt(jnp.full(SMALL, total / (ROWS * COLS), F32)))


FLOPS_PER_US = 10_000_000


def plain(kernel, outs, in_specs, out_specs, scratch, us, **kw):
    return pl.pallas_call(
        kernel, out_shape=outs, in_specs=in_specs, out_specs=out_specs, scratch_shapes=scratch,
        cost_estimate=pl.CostEstimate(flops=int(us * FLOPS_PER_US), bytes_accessed=1 << 20, transcendentals=0),
        compiler_params=pltpu.CompilerParams(vmem_limit_bytes=12 << 20), **kw)


def body(source):
    dma = pltpu.SemaphoreType.DMA
    x = source.reshape(HALVES, 8, TILES, 8, E, 2, 128).transpose(0, 1, 2, 4, 5, 3, 6)
    x = pltpu.with_memory_space_constraint(x, pltpu.HBM)
    landed = {}

    def permute(value, pairs):
        return lax.ppermute(value, AXES, pairs)

    def go(flows, *before):
        n = len(flows)
        pieces = plain(
            functools.partial(pack, flows), tuple(pltpu.VMEM((len(f[3]) * TILES, E, 8, 128), F32) for f in flows),
            [HBM] + [VMEM] * len(before), (VMEM,) * n, [dma((HALVES, n))], 1 + n / 3)(x, *before)
        for flow, piece in zip(flows, pieces):
            landed[flow] = permute(piece, permutation(flow))
        return pieces

    pieces = go(FIRST)
    pieces = go(SECOND, pieces[0])
    pieces = go(THIRD, pieces[0])
    tiles = functools.partial(pltpu.VMEM, dtype=F32)
    part = plain(reduce, tiles((2, *SMALL)), [HBM, VMEM], VMEM,
                 [pltpu.VMEM((SLOTS, TILES, E, 2, 8, 128), F32), dma((SLOTS,))], 7)(x, pieces[0])
    twin = permute(part, permutation((0, 0, 1)))
    both = plain(pair, tiles((2, *SMALL)), [VMEM] * 2, VMEM, [], 1)(part, twin)
    near = [permute(both, permutation(f)) for f in NEAR]
    plane = plain(gather, tiles((COL_PARTS, *SMALL)), [VMEM] * (1 + len(NEAR)), VMEM,
                  [tiles((COL_PARTS, ROW_PARTS, *SMALL))], 1)(both, *near)
    other = permute(plane, moved(lambda at: at | {"x1": 1 - at["x1"], "x0": 1 - at["x0"]}))
    sums, square = plain(
        combine, (tiles((E * COL_PARTS, 128)), tiles(SMALL)), [VMEM] * 2, (VMEM,) * 2, [], 1)(plane, other)
    stacked = [
        permute(square, moved(lambda at: at | {"z": (at["z"] + dz) % 4})) for dz in (1, 2, 3)]
    n = len(SOON)
    out = plain(
        write_soon, jax.ShapeDtypeStruct(BIG, F32), [HBM] + [VMEM] * n, HBM,
        [pltpu.VMEM((HALVES, TILES, E, 8, 128), F32), dma((2,)), dma((HALVES, n))], 5,
    )(x, *[landed[f] for f in SOON])
    columns, norm = plain(
        finish, (jax.ShapeDtypeStruct((E * COL_PARTS, 128), F32), jax.ShapeDtypeStruct((1, 1), F32)),
        [VMEM] * 5, (VMEM, pl.BlockSpec(memory_space=pltpu.SMEM)), [tiles((4, *SMALL))], 1)(sums, square, *stacked)
    for flows in GROUPS:
        n = len(flows)
        out = plain(
            functools.partial(write_group, flows), jax.ShapeDtypeStruct(BIG, F32), [HBM] + [VMEM] * n, HBM,
            [dma((HALVES, n))], 1, input_output_aliases={0: 0})(out, *[landed[f] for f in flows])
    return out.transpose(0, 1, 2, 5, 3, 4, 6).reshape(1024, 3072), columns.reshape(3072), norm.reshape(())


def solution(mesh):
    return jax.shard_map(body, mesh=mesh, in_specs=P("row", "col"), out_specs=(P("row", "col"), P("col"), P()),
                         check_vma=False)
```

```python
import functools

import jax
import jax.numpy as jnp
from jax import lax
from jax.experimental import pallas as pl
from jax.experimental.pallas import tpu as pltpu
from jax.sharding import PartitionSpec as P


AXES = ("row", "col")
ROWS, COLS = 16384, 24576
N_ROW, N_COL = 8, 16
HALVES, ROW_PARTS, TILES, E, COL_PARTS = 2, 4, 16, 6, 4
F32 = jnp.float32
WHOLE, UPPER, LOWER = (0, 1), (0,), (1,)
FIRST = [(0, 1, 0, WHOLE), (1, 1, 0, WHOLE)]
SECOND = [(0, 3, 0, WHOLE)]
THIRD = [(1, 2, 0, WHOLE), (1, 3, 0, WHOLE), (0, 1, 1, WHOLE), (0, 3, 1, WHOLE), (1, 1, 1, WHOLE), (0, 2, 0, WHOLE), (0, 2, 1, UPPER), (1, 3, 1, WHOLE), (0, 2, 1, LOWER), (0, 0, 1, WHOLE), (1, 2, 1, WHOLE), (1, 0, 0, WHOLE), (1, 0, 1, UPPER), (1, 0, 1, LOWER)]
NEAR = [(0, 1, 0), (0, 3, 0), (0, 2, 0), (1, 0, 0), (1, 1, 0), (1, 3, 0), (1, 2, 0)]
GROUPS = [[(1, 0, 0, WHOLE), (0, 1, 1, WHOLE)], [(0, 3, 1, WHOLE), (0, 2, 0, WHOLE)], [(0, 2, 1, UPPER), (1, 0, 1, UPPER)], [(0, 2, 1, LOWER), (1, 0, 1, LOWER)]]
SOON = [f for f in FIRST + SECOND + THIRD if f not in sum(GROUPS, [])]
SLOTS = 4
CHUNKS = HALVES * 8
VMEM = pl.BlockSpec(memory_space=pltpu.VMEM)
HBM = pl.BlockSpec(memory_space=pltpu.HBM)
SMALL = (8, 128)
BIG = (HALVES, ROW_PARTS, TILES, E, COL_PARTS, 8, 128)


def place(row, col):
    return {"x1": row // 4, "x0": (row // 2) % 2, "y": (col // 2) % 2 * 2 + row % 2, "z": col // 4, "core": col % 2}


def here():
    return place(lax.axis_index("row"), lax.axis_index("col"))


def shifted(at, flow, sign):
    dx, dy, dc = flow[:3]
    core = (at["core"] + dc) % 2
    turn = 1 - 2 * (at["core"] if sign > 0 else core)
    return at | {"x0": (at["x0"] + dx) % 2, "y": (at["y"] + sign * turn * dy + 4) % 4, "core": core}


def device(at):
    return at["x1"] * 4 + at["x0"] * 2 + at["y"] % 2, at["z"] * 4 + at["y"] // 2 * 2 + at["core"]


def row_part(at):
    return at["x0"] * 2 + at["y"] % 2


def col_part(at):
    return at["y"] // 2 * 2 + at["core"]


def slab(at):
    return at["y"] // 2 * 4 + at["x0"] * 2 + at["y"] % 2


def moved(target):
    pairs = []
    for row in range(N_ROW):
        for col in range(N_COL):
            to_row, to_col = device(target(place(row, col)))
            pairs.append((row * N_COL + col, to_row * N_COL + to_col))
    return pairs


def permutation(flow):
    return moved(lambda at: shifted(at, flow, 1))


def half(piece, i):
    return piece.at[i * TILES:(i + 1) * TILES]


def pack(flows, x_ref, *refs):
    n = len(flows)
    sem, outs = refs[-1], refs[len(refs) - 1 - n:-1]
    at = here()
    copies = []
    for k, flow in enumerate(flows):
        to = shifted(at, flow, 1)
        for i, c in enumerate(flow[3]):
            copies.append(pltpu.make_async_copy(x_ref.at[c, slab(to), :, :, to["core"]], half(outs[k], i), sem.at[i, k]))
            copies[-1].start()
    for copy in copies:
        copy.wait()


def reduce(x_ref, _, part_ref, chunk, sem):
    def load(n):
        return pltpu.make_async_copy(x_ref.at[n // 8, n % 8], chunk.at[n % SLOTS], sem.at[n % SLOTS])

    for n in range(SLOTS - 1):
        load(n).start()
    totals = (jnp.zeros((E, 2, 8, 128), F32), jnp.zeros((E, 2, 8, 128), F32))
    for n in range(CHUNKS):
        if n + SLOTS - 1 < CHUNKS:
            load(n + SLOTS - 1).start()
        load(n).wait()

        def add(t, totals, n=n):
            v = chunk[n % SLOTS, t]
            return totals[0] + v, totals[1] + v * v

        totals = lax.fori_loop(0, TILES, add, totals)
    by_column = jnp.sum(totals[0], axis=2)
    square = jnp.sum(totals[1], axis=(0, 1, 2), keepdims=True).reshape(1, 128)
    for c in range(2):
        part_ref[c, 0:E, :] = by_column[:, c]
        part_ref[c, E:E + 1, :] = square
        part_ref[c, E + 1:E + 2, :] = jnp.zeros((1, 128), F32)


def write(at, flows, pieces, out_ref, sem):
    copies = []
    for k, flow in enumerate(flows):
        by = shifted(at, flow, -1)
        for i, c in enumerate(flow[3]):
            copies.append(pltpu.make_async_copy(
                half(pieces[k], i), out_ref.at[c, row_part(by), :, :, col_part(by)], sem.at[i, k]))
            copies[-1].start()
    return copies


def pair(part, twin, both_ref):
    core = lax.axis_index("col") % 2
    both_ref[0] = part[core]
    both_ref[1] = twin[core]


def gather(*refs):
    plane_ref, parts = refs[-2:]
    at = here()
    for flow, both in zip([(0, 0, 0)] + NEAR, refs):
        by = shifted(at, flow, -1)
        parts[col_part(by), row_part(by)] = both[0]
        parts[col_part(by | {"core": 1 - at["core"]}), row_part(by)] = both[1]
    plane_ref[...] = parts[:, 0] + parts[:, 1] + parts[:, 2] + parts[:, 3]


def write_soon(x_ref, *refs):
    n = len(SOON)
    pieces, (out_ref, own, own_sem, sem) = refs[:n], refs[n:]
    at = here()
    load = pltpu.make_async_copy(x_ref.at[:, slab(at), :, :, at["core"]], own, own_sem.at[0])
    load.start()
    copies = write(at, SOON, pieces, out_ref, sem)
    load.wait()
    copies.append(pltpu.make_async_copy(own, out_ref.at[:, row_part(at), :, :, col_part(at)], own_sem.at[1]))
    copies[-1].start()
    for copy in copies:
        copy.wait()


def write_group(flows, _, *refs):
    pieces, (out_ref, sem) = refs[:len(flows)], refs[len(flows):]
    for copy in write(here(), flows, pieces, out_ref, sem):
        copy.wait()


def combine(plane_ref, other_ref, sums_ref, square_ref):
    whole = plane_ref[...] + other_ref[...]
    for e in range(E):
        sums_ref[e * COL_PARTS:(e + 1) * COL_PARTS, :] = whole[:, e] * (1.0 / 128.0)
    square_ref[...] = jnp.broadcast_to(whole[0, E] + whole[1, E] + whole[2, E] + whole[3, E], SMALL)


def finish(sums_ref, square_ref, z1, z2, z3, columns_ref, norm_ref, squares):
    z = lax.axis_index("col") // 4
    columns_ref[...] = sums_ref[...]
    for dz, ref in enumerate((square_ref, z1, z2, z3)):
        squares[(z - dz + 4) % 4] = ref[...]
    total = jnp.sum((squares[0] + squares[1] + squares[2] + squares[3])[0:1, :])
    norm_ref[0, 0] = jnp.max(jnp.sqrt(jnp.full(SMALL, total / (ROWS * COLS), F32)))


FLOPS_PER_US = 10_000_000


def plain(kernel, outs, in_specs, out_specs, scratch, us, **kw):
    return pl.pallas_call(
        kernel, out_shape=outs, in_specs=in_specs, out_specs=out_specs, scratch_shapes=scratch,
        cost_estimate=pl.CostEstimate(flops=int(us * FLOPS_PER_US), bytes_accessed=1 << 20, transcendentals=0),
        compiler_params=pltpu.CompilerParams(vmem_limit_bytes=12 << 20), **kw)


def body(source):
    dma = pltpu.SemaphoreType.DMA
    x = source.reshape(HALVES, 8, TILES, 8, E, 2, 128).transpose(0, 1, 2, 4, 5, 3, 6)
    x = pltpu.with_memory_space_constraint(x, pltpu.HBM)
    landed = {}

    def permute(value, pairs):
        return lax.ppermute(value, AXES, pairs)

    def go(flows, *before):
        n = len(flows)
        pieces = plain(
            functools.partial(pack, flows), tuple(pltpu.VMEM((len(f[3]) * TILES, E, 8, 128), F32) for f in flows),
            [HBM] + [VMEM] * len(before), (VMEM,) * n, [dma((HALVES, n))], 1 + n / 3)(x, *before)
        for flow, piece in zip(flows, pieces):
            landed[flow] = permute(piece, permutation(flow))
        return pieces

    pieces = go(FIRST)
    pieces = go(SECOND, pieces[0])
    pieces = go(THIRD, pieces[0])
    tiles = functools.partial(pltpu.VMEM, dtype=F32)
    part = plain(reduce, tiles((2, *SMALL)), [HBM, VMEM], VMEM,
                 [pltpu.VMEM((SLOTS, TILES, E, 2, 8, 128), F32), dma((SLOTS,))], 7)(x, pieces[0])
    twin = permute(part, permutation((0, 0, 1)))
    both = plain(pair, tiles((2, *SMALL)), [VMEM] * 2, VMEM, [], 1)(part, twin)
    near = [permute(both, permutation(f)) for f in NEAR]
    plane = plain(gather, tiles((COL_PARTS, *SMALL)), [VMEM] * (1 + len(NEAR)), VMEM,
                  [tiles((COL_PARTS, ROW_PARTS, *SMALL))], 1)(both, *near)
    other = permute(plane, moved(lambda at: at | {"x1": 1 - at["x1"], "x0": 1 - at["x0"]}))
    sums, square = plain(
        combine, (tiles((E * COL_PARTS, 128)), tiles(SMALL)), [VMEM] * 2, (VMEM,) * 2, [], 1)(plane, other)
    stacked = [
        permute(square, moved(lambda at: at | {"z": (at["z"] + dz) % 4})) for dz in (1, 2, 3)]
    n = len(SOON)
    out = plain(
        write_soon, jax.ShapeDtypeStruct(BIG, F32), [HBM] + [VMEM] * n, HBM,
        [pltpu.VMEM((HALVES, TILES, E, 8, 128), F32), dma((2,)), dma((HALVES, n))], 5,
    )(x, *[landed[f] for f in SOON])
    columns, norm = plain(
        finish, (jax.ShapeDtypeStruct((E * COL_PARTS, 128), F32), jax.ShapeDtypeStruct((1, 1), F32)),
        [VMEM] * 5, (VMEM, pl.BlockSpec(memory_space=pltpu.SMEM)), [tiles((4, *SMALL))], 1)(sums, square, *stacked)
    for flows in GROUPS:
        n = len(flows)
        out = plain(
            functools.partial(write_group, flows), jax.ShapeDtypeStruct(BIG, F32), [HBM] + [VMEM] * n, HBM,
            [dma((HALVES, n))], 1, input_output_aliases={0: 0})(out, *[landed[f] for f in flows])
    return out.transpose(0, 1, 2, 5, 3, 4, 6).reshape(1024, 3072), columns.reshape(3072), norm.reshape(())


def solution(mesh):
    return jax.shard_map(body, mesh=mesh, in_specs=P("row", "col"), out_specs=(P("row", "col"), P("col"), P()),
                         check_vma=False)
```

```python
import functools

import jax
import jax.numpy as jnp
from jax import lax
from jax.experimental import pallas as pl
from jax.experimental.pallas import tpu as pltpu
from jax.sharding import PartitionSpec as P


AXES = ("row", "col")
ROWS, COLS = 16384, 24576
N_ROW, N_COL = 8, 16
HALVES, ROW_PARTS, TILES, E, COL_PARTS = 2, 4, 16, 6, 4
F32 = jnp.float32
WHOLE, UPPER, LOWER = (0, 1), (0,), (1,)
FIRST = [(0, 1, 0, UPPER), (1, 1, 0, UPPER)]
SECOND = [(0, 3, 0, WHOLE), (1, 1, 0, LOWER), (0, 1, 0, LOWER)]
THIRD = [(1, 2, 0, WHOLE), (1, 3, 0, WHOLE), (0, 1, 1, WHOLE), (0, 3, 1, WHOLE), (1, 1, 1, WHOLE), (0, 2, 0, WHOLE), (0, 2, 1, UPPER), (1, 3, 1, WHOLE), (0, 2, 1, LOWER), (0, 0, 1, WHOLE), (1, 2, 1, WHOLE), (1, 0, 1, WHOLE), (1, 0, 0, UPPER), (1, 0, 0, LOWER)]
NEAR = [(0, 1, 0), (0, 3, 0), (0, 2, 0), (1, 0, 0), (1, 1, 0), (1, 3, 0), (1, 2, 0)]
GROUPS = [[(1, 0, 1, WHOLE), (0, 1, 1, WHOLE)], [(0, 3, 1, WHOLE), (0, 2, 0, WHOLE)], [(0, 2, 1, UPPER), (1, 0, 0, UPPER)], [(0, 2, 1, LOWER), (1, 0, 0, LOWER)]]
SOON = [f for f in FIRST + SECOND + THIRD if f not in sum(GROUPS, [])]
SLOTS = 4
CHUNKS = HALVES * 8
VMEM = pl.BlockSpec(memory_space=pltpu.VMEM)
HBM = pl.BlockSpec(memory_space=pltpu.HBM)
SMALL = (8, 128)
BIG = (HALVES, ROW_PARTS, TILES, E, COL_PARTS, 8, 128)


def place(row, col):
    return {"x1": row // 4, "x0": (row // 2) % 2, "y": (col // 2) % 2 * 2 + row % 2, "z": col // 4, "core": col % 2}


def here():
    return place(lax.axis_index("row"), lax.axis_index("col"))


def shifted(at, flow, sign):
    dx, dy, dc = flow[:3]
    core = (at["core"] + dc) % 2
    turn = 1 - 2 * (at["core"] if sign > 0 else core)
    return at | {"x0": (at["x0"] + dx) % 2, "y": (at["y"] + sign * turn * dy + 4) % 4, "core": core}


def device(at):
    return at["x1"] * 4 + at["x0"] * 2 + at["y"] % 2, at["z"] * 4 + at["y"] // 2 * 2 + at["core"]


def row_part(at):
    return at["x0"] * 2 + at["y"] % 2


def col_part(at):
    return at["y"] // 2 * 2 + at["core"]


def slab(at):
    return at["y"] // 2 * 4 + at["x0"] * 2 + at["y"] % 2


def moved(target):
    pairs = []
    for row in range(N_ROW):
        for col in range(N_COL):
            to_row, to_col = device(target(place(row, col)))
            pairs.append((row * N_COL + col, to_row * N_COL + to_col))
    return pairs


def permutation(flow):
    return moved(lambda at: shifted(at, flow, 1))


def half(piece, i):
    return piece.at[i * TILES:(i + 1) * TILES]


def pack(flows, x_ref, *refs):
    n = len(flows)
    sem, outs = refs[-1], refs[len(refs) - 1 - n:-1]
    at = here()
    copies = []
    for k, flow in enumerate(flows):
        to = shifted(at, flow, 1)
        for i, c in enumerate(flow[3]):
            copies.append(pltpu.make_async_copy(x_ref.at[c, slab(to), :, :, to["core"]], half(outs[k], i), sem.at[i, k]))
            copies[-1].start()
    for copy in copies:
        copy.wait()


def reduce(x_ref, _, part_ref, chunk, sem):
    def load(n):
        return pltpu.make_async_copy(x_ref.at[n // 8, n % 8], chunk.at[n % SLOTS], sem.at[n % SLOTS])

    for n in range(SLOTS - 1):
        load(n).start()
    totals = (jnp.zeros((E, 2, 8, 128), F32), jnp.zeros((E, 2, 8, 128), F32))
    for n in range(CHUNKS):
        if n + SLOTS - 1 < CHUNKS:
            load(n + SLOTS - 1).start()
        load(n).wait()

        def add(t, totals, n=n):
            v = chunk[n % SLOTS, t]
            return totals[0] + v, totals[1] + v * v

        totals = lax.fori_loop(0, TILES, add, totals)
    by_column = jnp.sum(totals[0], axis=2)
    square = jnp.sum(totals[1], axis=(0, 1, 2), keepdims=True).reshape(1, 128)
    for c in range(2):
        part_ref[c, 0:E, :] = by_column[:, c]
        part_ref[c, E:E + 1, :] = square
        part_ref[c, E + 1:E + 2, :] = jnp.zeros((1, 128), F32)


def write(at, flows, pieces, out_ref, sem):
    copies = []
    for k, flow in enumerate(flows):
        by = shifted(at, flow, -1)
        for i, c in enumerate(flow[3]):
            copies.append(pltpu.make_async_copy(
                half(pieces[k], i), out_ref.at[c, row_part(by), :, :, col_part(by)], sem.at[i, k]))
            copies[-1].start()
    return copies


def pair(part, twin, both_ref):
    core = lax.axis_index("col") % 2
    both_ref[0] = part[core]
    both_ref[1] = twin[core]


def gather(*refs):
    plane_ref, parts = refs[-2:]
    at = here()
    for flow, both in zip([(0, 0, 0)] + NEAR, refs):
        by = shifted(at, flow, -1)
        parts[col_part(by), row_part(by)] = both[0]
        parts[col_part(by | {"core": 1 - at["core"]}), row_part(by)] = both[1]
    plane_ref[...] = parts[:, 0] + parts[:, 1] + parts[:, 2] + parts[:, 3]


def write_soon(x_ref, *refs):
    n = len(SOON)
    pieces, (out_ref, own, own_sem, sem) = refs[:n], refs[n:]
    at = here()
    load = pltpu.make_async_copy(x_ref.at[:, slab(at), :, :, at["core"]], own, own_sem.at[0])
    load.start()
    copies = write(at, SOON, pieces, out_ref, sem)
    load.wait()
    copies.append(pltpu.make_async_copy(own, out_ref.at[:, row_part(at), :, :, col_part(at)], own_sem.at[1]))
    copies[-1].start()
    for copy in copies:
        copy.wait()


def write_group(flows, _, *refs):
    pieces, (out_ref, sem) = refs[:len(flows)], refs[len(flows):]
    for copy in write(here(), flows, pieces, out_ref, sem):
        copy.wait()


def combine(plane_ref, other_ref, sums_ref, square_ref):
    whole = plane_ref[...] + other_ref[...]
    for e in range(E):
        sums_ref[e * COL_PARTS:(e + 1) * COL_PARTS, :] = whole[:, e] * (1.0 / 128.0)
    square_ref[...] = jnp.broadcast_to(whole[0, E] + whole[1, E] + whole[2, E] + whole[3, E], SMALL)


def finish(sums_ref, square_ref, z1, z2, z3, columns_ref, norm_ref, squares):
    z = lax.axis_index("col") // 4
    columns_ref[...] = sums_ref[...]
    for dz, ref in enumerate((square_ref, z1, z2, z3)):
        squares[(z - dz + 4) % 4] = ref[...]
    total = jnp.sum((squares[0] + squares[1] + squares[2] + squares[3])[0:1, :])
    norm_ref[0, 0] = jnp.max(jnp.sqrt(jnp.full(SMALL, total / (ROWS * COLS), F32)))


FLOPS_PER_US = 10_000_000


def plain(kernel, outs, in_specs, out_specs, scratch, us, **kw):
    return pl.pallas_call(
        kernel, out_shape=outs, in_specs=in_specs, out_specs=out_specs, scratch_shapes=scratch,
        cost_estimate=pl.CostEstimate(flops=int(us * FLOPS_PER_US), bytes_accessed=1 << 20, transcendentals=0),
        compiler_params=pltpu.CompilerParams(vmem_limit_bytes=12 << 20), **kw)


def body(source):
    dma = pltpu.SemaphoreType.DMA
    x = source.reshape(HALVES, 8, TILES, 8, E, 2, 128).transpose(0, 1, 2, 4, 5, 3, 6)
    x = pltpu.with_memory_space_constraint(x, pltpu.HBM)
    landed = {}

    def permute(value, pairs):
        return lax.ppermute(value, AXES, pairs)

    def go(flows, *before):
        n = len(flows)
        pieces = plain(
            functools.partial(pack, flows), tuple(pltpu.VMEM((len(f[3]) * TILES, E, 8, 128), F32) for f in flows),
            [HBM] + [VMEM] * len(before), (VMEM,) * n, [dma((HALVES, n))], 1 + n / 3)(x, *before)
        for flow, piece in zip(flows, pieces):
            landed[flow] = permute(piece, permutation(flow))
        return pieces

    pieces = go(FIRST)
    pieces = go(SECOND, pieces[0])
    pieces = go(THIRD, pieces[0])
    tiles = functools.partial(pltpu.VMEM, dtype=F32)
    part = plain(reduce, tiles((2, *SMALL)), [HBM, VMEM], VMEM,
                 [pltpu.VMEM((SLOTS, TILES, E, 2, 8, 128), F32), dma((SLOTS,))], 7)(x, pieces[0])
    twin = permute(part, permutation((0, 0, 1)))
    both = plain(pair, tiles((2, *SMALL)), [VMEM] * 2, VMEM, [], 1)(part, twin)
    near = [permute(both, permutation(f)) for f in NEAR]
    plane = plain(gather, tiles((COL_PARTS, *SMALL)), [VMEM] * (1 + len(NEAR)), VMEM,
                  [tiles((COL_PARTS, ROW_PARTS, *SMALL))], 1)(both, *near)
    other = permute(plane, moved(lambda at: at | {"x1": 1 - at["x1"], "x0": 1 - at["x0"]}))
    sums, square = plain(
        combine, (tiles((E * COL_PARTS, 128)), tiles(SMALL)), [VMEM] * 2, (VMEM,) * 2, [], 1)(plane, other)
    stacked = [
        permute(square, moved(lambda at: at | {"z": (at["z"] + dz) % 4})) for dz in (1, 2, 3)]
    n = len(SOON)
    out = plain(
        write_soon, jax.ShapeDtypeStruct(BIG, F32), [HBM] + [VMEM] * n, HBM,
        [pltpu.VMEM((HALVES, TILES, E, 8, 128), F32), dma((2,)), dma((HALVES, n))], 5,
    )(x, *[landed[f] for f in SOON])
    columns, norm = plain(
        finish, (jax.ShapeDtypeStruct((E * COL_PARTS, 128), F32), jax.ShapeDtypeStruct((1, 1), F32)),
        [VMEM] * 5, (VMEM, pl.BlockSpec(memory_space=pltpu.SMEM)), [tiles((4, *SMALL))], 1)(sums, square, *stacked)
    for flows in GROUPS:
        n = len(flows)
        out = plain(
            functools.partial(write_group, flows), jax.ShapeDtypeStruct(BIG, F32), [HBM] + [VMEM] * n, HBM,
            [dma((HALVES, n))], 1, input_output_aliases={0: 0})(out, *[landed[f] for f in flows])
    return out.transpose(0, 1, 2, 5, 3, 4, 6).reshape(1024, 3072), columns.reshape(3072), norm.reshape(())


def solution(mesh):
    return jax.shard_map(body, mesh=mesh, in_specs=P("row", "col"), out_specs=(P("row", "col"), P("col"), P()),
                         check_vma=False)
```
